32 devices in a mesh: patch: 8 (over z, y), sub: 4 (over x, core).
Axes of the slice: x: 2, y: 2, z: 4, core: 2. Of those that a mesh axis runs over, the one named last changes fastest.
Arguments:
- sources: int32 [128, 2], replicated, may hold values from 0 to 16383
- diag_coef: float32 [16384], P(('patch', 'sub')), may hold values from 1 to 2
- tiles: float32 [128, 6, 128, 128], P(('patch', 'sub')), may hold values from -0.109375 to 0.109375
- tile_cols: int32 [128, 6], P(('patch', 'sub')), may hold values from 0 to 7
- send_rows: int32 [32, 4, 128], P(('patch', 'sub')), may hold values from 0 to 511
- recv_rows: int32 [32, 512], P(('patch', 'sub')), may hold values from 0 to 511, each once within a row
- bounds: float32 [2], replicated, may hold values from 0.3 to 3.2, as said below
Outputs:
- solution: float32 [16384, 128], P(('patch', 'sub'))
- res_norm: float32 [128], replicated
The draws below stay inside these ranges and needn't reach their ends.
Inputs may be any that keep to these rules, and one draw needn't show every extreme that they name: bounds[0] lies in 0.3 to 0.5 and bounds[1] in 2.6 to 3.2.
All inputs are finite; a program needn't handle non-finite values.
Results may differ from the reference program's by a relative error of at most 0.0001.
Values sent between devices are 32-bit elements; how exact they have to be, the bound alone decides.
A program may use at most 64 MiB of HBM per device.

```python
import jax
import jax.numpy as jnp
from jax import lax

BLOCK = 128
BLK_DEV = 4
NB = 6
K = 128
S = 128
ITERS = 8
V_DEV = 512
VERTS = 16384
BLOCKS = 128
H = 512
HB = 4
NSRC = 2
N_PATCH = 8
N_SUB = 4
DEVICES = 32


def draw_bounds(key, part):
    first_key, second_key = jax.random.split(key)
    lower_end = jax.random.uniform(first_key, (), jnp.float32, 0.3, 0.5)
    upper_end = jax.random.uniform(second_key, (), jnp.float32, 2.6, 3.2)
    return jnp.stack([lower_end, upper_end]).astype(jnp.float32)


def with_ends(drawn, own_key, smallest, largest):
    longest = drawn.shape.index(max(drawn.shape))
    spots = []
    for shift in (0, 1):
        where = [jax.random.randint(jax.random.fold_in(own_key, axis), (), 0, length) for axis, length in enumerate(drawn.shape)]
        where[longest] = (where[longest] + shift) % drawn.shape[longest]
        spots.append(tuple(where))
    return drawn.at[spots[0]].set(smallest).at[spots[1]].set(largest)


def block_scale(rng, extent, cuts, low, high):
    def one(position, shards_of):
        draws = jax.random.uniform(jax.random.fold_in(jax.random.fold_in(rng, 6), position), (shards_of,), jnp.float32, low / len(cuts), high / len(cuts))
        return jnp.repeat(jnp.exp(draws), extent[position] // shards_of).reshape((-1,) + (1,) * (len(extent) - position - 1))

    level = one(*cuts[0])
    for cut in cuts[1:]:
        level = level * one(*cut)
    return level


def noise(key, dims, width, most, pieces=(), held_as=jnp.bfloat16):
    values = width * jax.random.normal(key, dims, jnp.float32)
    if pieces:
        values = values * block_scale(key, dims, pieces, -0.22, 0.18)
    return jnp.clip(values, -most, most).astype(held_as)


def setup_inputs(seed: int = 0) -> dict:
    keys = jax.random.split(jax.random.key(seed), 8)
    sources = with_ends(jax.random.randint(keys[0], (K, NSRC), 0, VERTS), jax.random.fold_in(keys[0], 1), 0, VERTS - 1).astype(jnp.int32)
    diag_coef = jnp.clip(1.0 + 1.0 * jax.random.uniform(keys[1], (VERTS,), jnp.float32) ** block_scale(keys[1], (VERTS,), ((0, 32),), -0.2, 0.2), 1.0, 2.0)
    tiles = noise(keys[2], (BLOCKS, NB, BLOCK, BLOCK), (4 * NB * BLOCK) ** -0.5, 0.109375, ((0, 32),), jnp.float32)
    tile_cols = with_ends(jax.random.randint(keys[3], (BLOCKS, NB), 0, BLK_DEV + HB), jax.random.fold_in(keys[3], 1), 0, (BLK_DEV + HB) - 1).astype(jnp.int32)
    send_rows = with_ends(jax.random.randint(keys[4], (DEVICES, 4, S), 0, V_DEV), jax.random.fold_in(keys[4], 1), 0, V_DEV - 1).astype(jnp.int32)
    recv_rows = jax.vmap(lambda own: jax.random.permutation(own, H))(jax.random.split(keys[5], DEVICES)).reshape((DEVICES, H)).astype(jnp.int32)
    bounds = draw_bounds(jax.random.fold_in(keys[7], 71), 0)
    return dict(sources=sources, diag_coef=diag_coef, tiles=tiles, tile_cols=tile_cols, send_rows=send_rows, recv_rows=recv_rows, bounds=bounds)


def build_right(sources, total_rows):
    columns = sources.shape[0]
    which = jnp.arange(columns, dtype=jnp.int32)[:, None]
    flat_index = (sources * columns + which).reshape(-1)
    counts = jax.ops.segment_sum(jnp.ones(flat_index.shape, jnp.float32), flat_index, num_segments=total_rows * columns)
    return counts.reshape(total_rows, columns)

def pick_rows(values, index):
    return values[index]

def operate(field, diag_coef, tiles, tile_cols, send_rows, recv_rows):
    devices = N_PATCH * N_SUB
    rows = BLK_DEV * BLOCK
    columns = field.shape[1]
    local = field.reshape(devices, rows, columns)
    packed = jax.vmap(pick_rows)(local, send_rows)
    packed = packed.reshape(N_PATCH, N_SUB, 4, S, columns)
    below_patch = jnp.roll(packed[:, :, 1], 1, axis=0)
    above_patch = jnp.roll(packed[:, :, 0], -1, axis=0)
    below_sub = jnp.roll(packed[:, :, 3], 1, axis=1)
    above_sub = jnp.roll(packed[:, :, 2], -1, axis=1)
    received = jnp.concatenate([below_patch, above_patch, below_sub, above_sub], axis=2)
    received = received.reshape(devices, 4 * S, columns)
    halo_rows = jax.vmap(pick_rows)(received, recv_rows)
    extended = jnp.concatenate([local, halo_rows], axis=1).reshape(devices, BLK_DEV + HB, BLOCK, columns)
    tile_blocks = tiles.reshape(devices, BLK_DEV, NB, BLOCK, BLOCK)
    col_blocks = tile_cols.reshape(devices, BLK_DEV, NB)

    def device_product(inputs):
        dev_tiles, dev_cols, dev_ext = inputs
        summed = jnp.zeros((BLK_DEV, BLOCK, columns), jnp.float32)
        for slot_index in range(NB):
            summed = summed + jnp.einsum('bij,bjk->bik', dev_tiles[:, slot_index], dev_ext[dev_cols[:, slot_index]], precision=lax.Precision.HIGHEST)
        return summed
    coupled = lax.map(device_product, (tile_blocks, col_blocks, extended)).reshape(devices * rows, columns)
    return diag_coef[:, None] * field + coupled

def reference(sources, diag_coef, tiles, tile_cols, send_rows, recv_rows, bounds):
    right_side = build_right(sources, VERTS)
    centre = (bounds[0] + bounds[1]) / 2.0
    half_width = (bounds[1] - bounds[0]) / 2.0
    ratio = centre / half_width
    damping = 1.0 / ratio
    solution = jnp.zeros_like(right_side)
    residual = right_side
    direction = right_side / centre
    for iteration in range(ITERS):
        solution = solution + direction
        residual = residual - operate(direction, diag_coef, tiles, tile_cols, send_rows, recv_rows)
        if iteration + 1 < ITERS:
            damping_next = 1.0 / (2.0 * ratio - damping)
            direction = damping_next * damping * direction + 2.0 * damping_next / half_width * residual
            damping = damping_next
    final = right_side - operate(solution, diag_coef, tiles, tile_cols, send_rows, recv_rows)
    res_norm = jnp.sqrt(lax.optimization_barrier(jnp.sum(final * final, axis=0)))
    return (solution, res_norm)
```

```python
import functools

import jax
import jax.numpy as jnp
from jax import lax
from jax.experimental import pallas as pl
from jax.experimental.pallas import tpu as pltpu
from jax.sharding import PartitionSpec as P

ITERS = 8
MESH = pl.DeviceIdType.MESH
F32 = jnp.float32
BF16 = jnp.bfloat16


def halves(value):
    high = value.astype(BF16)
    return high, (value - high.astype(F32)).astype(BF16)


def product(high, low, pair, columns):
    wide = jnp.dot(high, pair, preferred_element_type=F32)
    narrow = jnp.dot(low, pair[:, :columns], preferred_element_type=F32)
    return wide[:, :columns] + wide[:, columns:] + narrow


def exact(high, low, counts):
    return jnp.dot(high, counts, preferred_element_type=F32) + jnp.dot(
        low, counts, preferred_element_type=F32
    )


def kernel(
    n_patch, n_sub,
    sources_hbm, diag_hbm, tiles_hbm, cols_hbm, sends_hbm, receives_hbm, bounds_hbm,
    solution_ref, norm_ref,
    sources_ref, diag_ref, cols_ref, sends_ref, receives_ref, bounds_ref,
    tiles_ref, near_hi, near_lo, far_hi, far_lo, halo_hi, halo_lo,
    near_first_hi, near_first_lo, far_first_hi, far_first_lo,
    direction_ref, residual_ref, packed_residual, total_ref, own_total, pair_ref, heard_pair,
    packed_ref, message_ref, heard_ref, heard_rows, heard_counts, norms_ref, counts_ref,
    packed_counts, pick_ref, place_ref, keeps_ref, gains_ref,
    back_hi, back_lo, echo_out, echo_in, echo_hi, echo_lo, echo_ref,
    input_sems, tile_sems, row_send, row_recv, echo_sems,
    send_sems, recv_sems, norm_send, norm_recv,
):
    blk_rows, per_row, size, _ = tiles_hbm.shape
    rows = blk_rows * size
    n_src, columns = sources_ref.shape
    sent = sends_ref.shape[2]
    halo = receives_ref.shape[1]
    packed_rows = 4 * sent
    patch, sub = lax.axis_index("patch"), lax.axis_index("sub")
    devices = n_patch * n_sub
    me = patch * n_sub + sub
    patch_odd, sub_odd = lax.rem(patch, 2), lax.rem(sub, 2)

    partners = [
        (lax.rem(patch + n_patch - 1 + 2 * patch_odd, n_patch), sub),
        (lax.rem(patch + n_patch + 1 - 2 * patch_odd, n_patch), sub),
        (patch, lax.rem(sub + n_sub - 1 + 2 * sub_odd, n_sub)),
        (patch, lax.rem(sub + n_sub + 1 - 2 * sub_odd, n_sub)),
    ]
    sides = [patch_odd, 1 - patch_odd, 2 + sub_odd, 3 - sub_odd]
    spans = [pl.ds(g * sent, sent) for g in range(4)]

    barrier = pltpu.get_barrier_semaphore()
    if n_patch // 2 + n_sub // 2 <= ITERS:
        for partner in partners:
            pl.semaphore_signal(barrier, inc=1, device_id=partner, device_id_type=MESH)
        awaited = 4
    else:
        @pl.loop(1, devices)
        def _(step):
            other = lax.rem(me + step, devices)
            pl.semaphore_signal(
                barrier, inc=1, device_id=(other // n_sub, lax.rem(other, n_sub)), device_id_type=MESH
            )
        awaited = devices - 1

    inputs = [
        pltpu.make_async_copy(source, target, input_sems.at[i])
        for i, (source, target) in enumerate((
            (sends_hbm, sends_ref), (receives_hbm, receives_ref), (sources_hbm, sources_ref),
            (cols_hbm, cols_ref), (diag_hbm, diag_ref), (bounds_hbm, bounds_ref),
        ))
    ]
    for copy in inputs:
        copy.start()
    copies = [
        pltpu.make_async_copy(tiles_hbm.at[b], tiles_ref.at[b], tile_sems.at[b])
        for b in range(blk_rows)
    ]
    for copy in copies:
        copy.start()
    for copy in inputs:
        copy.wait()

    low_end = jnp.full((1, columns), bounds_ref[0], F32)
    high_end = jnp.full((1, columns), bounds_ref[1], F32)
    centre = (low_end + high_end) / 2.0
    half_width = (high_end - low_end) / 2.0
    ratio = centre / half_width
    damping = 1.0 / ratio
    for k in range(ITERS - 1):
        damping_next = 1.0 / (2.0 * ratio - damping)
        keeps_ref[k] = damping_next * damping
        gains_ref[k] = 2.0 * damping_next / half_width
        damping = damping_next

    def counted(ids):
        total = jnp.zeros(ids.shape, F32)
        for s in range(n_src):
            total = total + jnp.where(sources_ref[s : s + 1, :] == ids, 1.0, 0.0)
        return total

    counts_ref[...] = counted(
        me * rows + lax.broadcasted_iota(jnp.int32, (rows, columns), 0)
    ).astype(BF16)

    def as_column(row, width):
        return jnp.broadcast_to(row, (width, row.shape[1])).T

    for g in range(4):
        wide = as_column(sends_ref[sides[g]], rows)
        pick_ref[spans[g]] = jnp.where(
            wide == lax.broadcasted_iota(jnp.int32, (sent, rows), 1), 1.0, 0.0
        ).astype(BF16)
    for i in range(halo // size):
        wide = as_column(receives_ref[:, i * size : (i + 1) * size], sent)
        for g in range(4):
            place_ref[pl.ds(i * size, size), spans[g]] = jnp.where(
                wide == sides[g] * sent + lax.broadcasted_iota(jnp.int32, (size, sent), 1), 1.0, 0.0
            ).astype(BF16)

    eye = lax.broadcasted_iota(jnp.int32, (size, size), 0) == lax.broadcasted_iota(
        jnp.int32, (size, size), 1
    )
    for b in range(blk_rows):
        copies[b].wait()
        for c in range(blk_rows + halo // size):
            block = jnp.zeros((size, size), F32)
            for n in range(per_row):
                block = block + tiles_ref[b, n] * (cols_ref[b, n] == c).astype(F32)
            if c == b:
                block = block + jnp.where(eye, diag_ref[b : b + 1, :], 0.0)
            high, low = halves(block)
            at = pl.ds(b * size, size)
            if c < blk_rows:
                near_hi[at, pl.ds(c * size, size)] = high
                near_lo[at, pl.ds(c * size, size)] = low
            else:
                place_at = pl.ds((c - blk_rows) * size, size)
                halo_hi[at, place_at] = high
                halo_lo[at, place_at] = low

    pl.semaphore_wait(barrier, awaited)

    def row_copy(g):
        return pltpu.make_async_remote_copy(
            src_ref=sends_ref.at[sides[g]], dst_ref=heard_rows.at[g],
            send_sem=row_send.at[g], recv_sem=row_recv.at[g],
            device_id=partners[g], device_id_type=MESH,
        )

    for g in range(4):
        row_copy(g).start()

    def chosen(matrix):
        return jnp.dot(pick_ref[...], matrix[...], preferred_element_type=F32).astype(BF16)

    for halo_part, far in ((halo_hi, far_hi), (halo_lo, far_lo)):
        far[...] = jnp.dot(
            halo_part[...], place_ref[...], preferred_element_type=F32
        ).astype(BF16)
    far_first_hi[...] = chosen(far_hi)
    far_first_lo[...] = chosen(far_lo)

    first, others = spans[0], pl.ds(sent, 3 * sent)
    back_hi[...] = far_first_hi[first, first]
    back_lo[...] = far_first_lo[first, first]
    echo_out[...] = back_hi[...].astype(F32) + back_lo[...].astype(F32)
    echo_copy = pltpu.make_async_remote_copy(
        src_ref=echo_out, dst_ref=echo_in, send_sem=echo_sems.at[0], recv_sem=echo_sems.at[1],
        device_id=partners[0], device_id_type=MESH,
    )
    echo_copy.start()
    near_first_hi[...] = chosen(near_hi)
    near_first_lo[...] = chosen(near_lo)
    packed_counts[...] = jnp.dot(pick_ref[...], counts_ref[...], preferred_element_type=F32)
    total_ref[...] = exact(near_first_hi[...], near_first_lo[...], counts_ref[...])

    def hear_counts(g):
        row_copy(g).wait_recv()
        base = (partners[g][0] * n_sub + partners[g][1]) * rows
        heard_counts[spans[g]] = counted(base + as_column(heard_rows[g], columns)).astype(BF16)

    def mail(source, slot, g):
        return pltpu.make_async_remote_copy(
            src_ref=source, dst_ref=heard_ref.at[slot, g],
            send_sem=send_sems.at[slot, g], recv_sem=recv_sems.at[slot, g],
            device_id=partners[g], device_id_type=MESH,
        )

    def hear(slot, g):
        mail(packed_ref.at[slot, g], slot, g).wait_recv()
        value = heard_ref[slot, g]
        if g == 0:
            value = value - echo_ref[...]
        high, low = halves(value)
        heard_pair[spans[g], :columns] = high
        heard_pair[spans[g], columns:] = low

    for g in (3, 2, 1, 0):
        hear_counts(g)
    keep, gain = keeps_ref[0], gains_ref[0]
    total = total_ref[...] + exact(far_first_hi[...], far_first_lo[...], heard_counts[...])
    rest = packed_counts[...] - total / centre
    packed_residual[...] = rest
    fresh = keep * (packed_counts[...] / centre) + gain * rest
    for g in range(4):
        packed_ref[1, g] = fresh[g * sent : (g + 1) * sent]
    for g in range(4):
        mail(packed_ref.at[1, g], 1, g).start()

    def send_direction(direction):
        direction_ref[...] = direction
        high, low = halves(direction)
        pair_ref[:, :columns] = high
        pair_ref[:, columns:] = low

    right_side = counts_ref[...].astype(F32)
    total = exact(near_hi[...], near_lo[...], counts_ref[...]) + exact(
        far_hi[...], far_lo[...], heard_counts[...]
    )
    residual = right_side - total / centre
    residual_ref[...] = residual
    before = right_side / centre
    direction = keep * before + gain * residual
    solution_ref[...] = before + direction
    send_direction(direction)

    far_first_hi[first, first] = jnp.zeros((sent, sent), BF16)
    far_first_lo[first, first] = jnp.zeros((sent, sent), BF16)
    echo_ref[...] = jnp.zeros((sent, columns), F32)
    echo_copy.wait()
    echo_hi[...], echo_lo[...] = halves(echo_in[...])

    def far_product(at, part):
        return product(far_first_hi[at, part], far_first_lo[at, part], heard_pair[part], columns)

    def step(slot):
        keep, gain = keeps_ref[slot], gains_ref[slot]
        total_ref[...] = product(near_first_hi[...], near_first_lo[...], pair_ref[...], columns)
        hear(slot, 3)
        everything, middle = pl.ds(0, packed_rows), pl.ds(sent, 2 * sent)
        total_ref[...] = total_ref[...] + far_product(everything, spans[3])
        hear(slot, 2)
        hear(slot, 1)
        rest = packed_residual[first] - (total_ref[first] + far_product(first, middle))
        packed_residual[first] = rest
        message_ref[slot + 1] = keep * packed_ref[slot, 0] + gain * rest
        mail(message_ref.at[slot + 1], slot + 1, 0).start()
        total_ref[others] = total_ref[others] + far_product(others, middle)
        hear(slot, 0)
        rest = packed_residual[others] - (total_ref[others] + far_product(others, first))
        packed_residual[others] = rest
        for g in (1, 2, 3):
            packed_ref[slot + 1, g] = (
                keep * packed_ref[slot, g] + gain * rest[(g - 1) * sent : g * sent]
            )
        for g in (1, 2, 3):
            mail(packed_ref.at[slot + 1, g], slot + 1, g).start()

        residual = residual_ref[...] - (
            product(near_hi[...], near_lo[...], pair_ref[...], columns)
            + product(far_hi[...], far_lo[...], heard_pair[...], columns)
        )
        residual_ref[...] = residual
        direction = keep * direction_ref[...] + gain * residual
        solution_ref[...] = solution_ref[...] + direction
        send_direction(direction)
        rest = packed_residual[first] - product(back_hi[...], back_lo[...], heard_pair[first], columns)
        packed_residual[first] = rest
        packed_ref[slot + 1, 0] = keep * packed_ref[slot, 0] + gain * rest
        high, low = halves(packed_ref[slot, 0])
        echo_ref[...] = gain * product(
            echo_hi[...], echo_lo[...], jnp.concatenate([high, low], axis=1), columns
        )

    lax.fori_loop(1, ITERS - 1, lambda slot, _: (step(slot), 0)[1], 0)

    slot = ITERS - 1
    total = product(near_hi[...], near_lo[...], pair_ref[...], columns)
    own_total[...] = residual_ref[...] - total
    for groups in ((3,), (2,), (1, 0)):
        for g in groups:
            hear(slot, g)
        part = pl.ds(groups[-1] * sent, len(groups) * sent)
        total = product(far_hi[:, part], far_lo[:, part], heard_pair[part], columns)
        if groups[-1]:
            own_total[...] = own_total[...] - total
    final = own_total[...] - total
    norms_ref[me] = jnp.sum(final * final, axis=0, keepdims=True)

    @pl.loop(1, devices)
    def _(step):
        other = lax.rem(me + step, devices)
        pltpu.make_async_remote_copy(
            src_ref=norms_ref.at[me], dst_ref=norms_ref.at[me],
            send_sem=norm_send, recv_sem=norm_recv,
            device_id=(other // n_sub, lax.rem(other, n_sub)), device_id_type=MESH,
        ).start()

    for g in range(4):
        row_copy(g).wait_send()
        for slot in range(1, ITERS):
            mail(packed_ref.at[slot, g], slot, g).wait_send()
    parts = norms_ref.at[pl.ds(0, devices - 1)]
    pltpu.make_async_copy(parts, parts, norm_recv).wait()
    pltpu.make_async_copy(parts, parts, norm_send).wait()
    norm_ref[...] = jnp.sqrt(jnp.sum(norms_ref[...], axis=0))


def finish(held_ref, norm_ref, result_hbm, root_hbm, sems):
    copies = [
        pltpu.make_async_copy(held_ref, result_hbm, sems.at[0]),
        pltpu.make_async_copy(norm_ref, root_hbm, sems.at[1]),
    ]
    for copy in copies:
        copy.start()
    for copy in copies:
        copy.wait()


def solution(mesh):
    n_patch, n_sub = mesh.shape["patch"], mesh.shape["sub"]

    def on_device(sources, diag_coef, tiles, tile_cols, send_rows, recv_rows, bounds):
        blk_rows, per_row, size, _ = tiles.shape
        rows = diag_coef.shape[0]
        columns = sources.shape[0]
        n_src = sources.shape[1]
        sent = send_rows.shape[2]
        halo = recv_rows.shape[1]
        packed = 4 * sent
        vmem, smem = pltpu.VMEM, pltpu.SMEM
        dma = pltpu.SemaphoreType.DMA
        anywhere = pl.BlockSpec(memory_space=pl.ANY)
        held, norm = pl.pallas_call(
            functools.partial(kernel, n_patch, n_sub),
            out_shape=(vmem((rows, columns), F32), vmem((1, columns), F32)),
            in_specs=[anywhere] * 7,
            out_specs=(pl.BlockSpec(memory_space=vmem), pl.BlockSpec(memory_space=vmem)),
            scratch_shapes=[
                vmem((n_src, columns), jnp.int32),
                vmem((blk_rows, size), F32),
                smem((blk_rows, per_row), jnp.int32),
                vmem((4, 1, sent), jnp.int32),
                vmem((1, halo), jnp.int32),
                smem((2,), F32),
                vmem(tiles.shape, F32),
                vmem((rows, rows), BF16),
                vmem((rows, rows), BF16),
                vmem((rows, packed), BF16),
                vmem((rows, packed), BF16),
                vmem((rows, halo), BF16),
                vmem((rows, halo), BF16),
                vmem((packed, rows), BF16),
                vmem((packed, rows), BF16),
                vmem((packed, packed), BF16),
                vmem((packed, packed), BF16),
                vmem((rows, columns), F32),
                vmem((rows, columns), F32),
                vmem((packed, columns), F32),
                vmem((packed, columns), F32),
                vmem((rows, columns), F32),
                vmem((rows, 2 * columns), BF16),
                vmem((packed, 2 * columns), BF16),
                vmem((ITERS, 4, sent, columns), F32),
                vmem((ITERS, sent, columns), F32),
                vmem((ITERS, 4, sent, columns), F32),
                vmem((4, 1, sent), jnp.int32),
                vmem((packed, columns), BF16),
                vmem((n_patch * n_sub, 1, columns), F32),
                vmem((rows, columns), BF16),
                vmem((packed, columns), F32),
                vmem((packed, rows), BF16),
                vmem((halo, packed), BF16),
                vmem((ITERS, 1, columns), F32),
                vmem((ITERS, 1, columns), F32),
                vmem((sent, sent), BF16),
                vmem((sent, sent), BF16),
                vmem((sent, sent), F32),
                vmem((sent, sent), F32),
                vmem((sent, sent), BF16),
                vmem((sent, sent), BF16),
                vmem((sent, columns), F32),
                dma((6,)),
                dma((blk_rows,)),
                dma((4,)),
                dma((4,)),
                dma((2,)),
                dma((ITERS, 4)),
                dma((ITERS, 4)),
                dma,
                dma,
            ],
            compiler_params=pltpu.CompilerParams(collective_id=0, has_side_effects=True),
            name="chebyshev",
        )(
            sources.T,
            diag_coef.reshape(blk_rows, size),
            tiles,
            tile_cols,
            send_rows.reshape(4, 1, sent),
            recv_rows,
            bounds,
        )
        result, root = pl.pallas_call(
            finish,
            out_shape=(
                jax.ShapeDtypeStruct((rows, columns), F32),
                jax.ShapeDtypeStruct((1, columns), F32),
            ),
            in_specs=[pl.BlockSpec(memory_space=vmem)] * 2,
            out_specs=(anywhere, anywhere),
            scratch_shapes=[dma((2,))],
            name="finish",
        )(pltpu.with_memory_space_constraint(held, vmem), pltpu.with_memory_space_constraint(norm, vmem))
        return result, root.reshape(columns)

    return jax.shard_map(
        on_device,
        mesh=mesh,
        in_specs=(
            P(),
            P(("patch", "sub")),
            P(("patch", "sub"), None, None, None),
            P(("patch", "sub"), None),
            P(("patch", "sub"), None, None),
            P(("patch", "sub"), None),
            P(),
        ),
        out_specs=(P(("patch", "sub"), None), P()),
        check_vma=False,
    )
```

```python
import functools

import jax
import jax.numpy as jnp
from jax import lax
from jax.experimental import pallas as pl
from jax.experimental.pallas import tpu as pltpu
from jax.sharding import PartitionSpec as P

ITERS = 8
MESH = pl.DeviceIdType.MESH
F32 = jnp.float32
BF16 = jnp.bfloat16


def halves(value):
    high = value.astype(BF16)
    return high, (value - high.astype(F32)).astype(BF16)


def product(high, low, mixed_pair):
    return jnp.dot(high, mixed_pair, preferred_element_type=F32) + jnp.dot(
        low, mixed_pair, preferred_element_type=F32
    )


def whole(high, low, pair):
    columns = pair.shape[1] // 2
    wide = jnp.dot(high, pair, preferred_element_type=F32)
    narrow = jnp.dot(low, pair[:, :columns], preferred_element_type=F32)
    return wide[:, :columns] + wide[:, columns:] + narrow


def turn(value):
    return pltpu.roll(value, value.shape[1] // 2, 1)


def in_left(value):
    lanes = lax.broadcasted_iota(jnp.int32, value.shape, 1)
    return lanes < value.shape[1] // 2


def doubled(value):
    other, left = turn(value), in_left(value)
    return jnp.where(left, value, other), jnp.where(left, other, value)


def fold(wide):
    return wide + turn(wide)


def exact(high, low, counts):
    return jnp.dot(high, counts, preferred_element_type=F32) + jnp.dot(
        low, counts, preferred_element_type=F32
    )


def kernel(
    n_patch, n_sub,
    sources_hbm, diag_hbm, tiles_hbm, cols_hbm, sends_hbm, receives_hbm, bounds_hbm,
    solution_ref, norm_ref,
    sources_ref, diag_ref, cols_ref, sends_ref, receives_ref, bounds_ref,
    tiles_ref, near_hi, near_lo, far_hi, far_lo, halo_hi, halo_lo,
    near_first_hi, near_first_lo, far_first_hi, far_first_lo,
    direction_ref, residual_ref, packed_residual, packed_direction, total_ref, totals_ref, own_total, pair_ref, heard_pair, heard_mixed,
    outbox_ref, heard_ref, heard_rows, heard_counts, norms_ref, counts_ref,
    packed_counts, pick_ref, place_ref, keeps_ref, gains_ref,
    back_hi, back_lo, echo_out, echo_in, echo_hi, echo_lo, echo_ref,
    input_sems, tile_sems, row_send, row_recv, echo_sems,
    send_sems, recv_sems, norm_send, norm_recv,
):
    blk_rows, per_row, size, _ = tiles_hbm.shape
    rows = blk_rows * size
    n_src, columns = sources_ref.shape
    sent = sends_ref.shape[2]
    halo = receives_ref.shape[1]
    packed_rows = 4 * sent
    patch, sub = lax.axis_index("patch"), lax.axis_index("sub")
    devices = n_patch * n_sub
    me = patch * n_sub + sub
    patch_odd, sub_odd = lax.rem(patch, 2), lax.rem(sub, 2)

    partners = [
        (lax.rem(patch + n_patch - 1 + 2 * patch_odd, n_patch), sub),
        (lax.rem(patch + n_patch + 1 - 2 * patch_odd, n_patch), sub),
        (patch, lax.rem(sub + n_sub - 1 + 2 * sub_odd, n_sub)),
        (patch, lax.rem(sub + n_sub + 1 - 2 * sub_odd, n_sub)),
    ]
    sides = [patch_odd, 1 - patch_odd, 2 + sub_odd, 3 - sub_odd]
    spans = [pl.ds(g * sent, sent) for g in range(4)]

    barrier = pltpu.get_barrier_semaphore()
    if n_patch // 2 + n_sub // 2 <= ITERS:
        for partner in partners:
            pl.semaphore_signal(barrier, inc=1, device_id=partner, device_id_type=MESH)
        awaited = 4
    else:
        @pl.loop(1, devices)
        def _(step):
            other = lax.rem(me + step, devices)
            pl.semaphore_signal(
                barrier, inc=1, device_id=(other // n_sub, lax.rem(other, n_sub)), device_id_type=MESH
            )
        awaited = devices - 1

    inputs = [
        pltpu.make_async_copy(source, target, input_sems.at[i])
        for i, (source, target) in enumerate((
            (sends_hbm, sends_ref), (receives_hbm, receives_ref), (sources_hbm, sources_ref),
            (cols_hbm, cols_ref), (diag_hbm, diag_ref), (bounds_hbm, bounds_ref),
        ))
    ]
    for copy in inputs:
        copy.start()
    copies = [
        pltpu.make_async_copy(tiles_hbm.at[b], tiles_ref.at[b], tile_sems.at[b])
        for b in range(blk_rows)
    ]
    for copy in copies:
        copy.start()
    for copy in inputs:
        copy.wait()

    low_end = jnp.full((1, columns), bounds_ref[0], F32)
    high_end = jnp.full((1, columns), bounds_ref[1], F32)
    centre = (low_end + high_end) / 2.0
    half_width = (high_end - low_end) / 2.0
    ratio = centre / half_width
    damping = 1.0 / ratio
    for k in range(ITERS - 1):
        damping_next = 1.0 / (2.0 * ratio - damping)
        keeps_ref[k] = damping_next * damping
        gains_ref[k] = 2.0 * damping_next / half_width
        damping = damping_next

    def counted(ids):
        total = jnp.zeros(ids.shape, F32)
        for s in range(n_src):
            total = total + jnp.where(sources_ref[s : s + 1, :] == ids, 1.0, 0.0)
        return total

    counts_ref[...] = counted(
        me * rows + lax.broadcasted_iota(jnp.int32, (rows, columns), 0)
    ).astype(BF16)

    def as_column(row, width):
        return jnp.broadcast_to(row, (width, row.shape[1])).T

    for g in range(4):
        wide = as_column(sends_ref[sides[g]], rows)
        pick_ref[spans[g]] = jnp.where(
            wide == lax.broadcasted_iota(jnp.int32, (sent, rows), 1), 1.0, 0.0
        ).astype(BF16)
    for i in range(halo // size):
        wide = as_column(receives_ref[:, i * size : (i + 1) * size], sent)
        for g in range(4):
            place_ref[pl.ds(i * size, size), spans[g]] = jnp.where(
                wide == sides[g] * sent + lax.broadcasted_iota(jnp.int32, (size, sent), 1), 1.0, 0.0
            ).astype(BF16)

    eye = lax.broadcasted_iota(jnp.int32, (size, size), 0) == lax.broadcasted_iota(
        jnp.int32, (size, size), 1
    )
    for b in range(blk_rows):
        copies[b].wait()
        for c in range(blk_rows + halo // size):
            block = jnp.zeros((size, size), F32)
            for n in range(per_row):
                block = block + tiles_ref[b, n] * (cols_ref[b, n] == c).astype(F32)
            if c == b:
                block = block + jnp.where(eye, diag_ref[b : b + 1, :], 0.0)
            high, low = halves(block)
            at = pl.ds(b * size, size)
            if c < blk_rows:
                near_hi[at, pl.ds(c * size, size)] = high
                near_lo[at, pl.ds(c * size, size)] = low
            else:
                place_at = pl.ds((c - blk_rows) * size, size)
                halo_hi[at, place_at] = high
                halo_lo[at, place_at] = low

    pl.semaphore_wait(barrier, awaited)

    def row_copy(g):
        return pltpu.make_async_remote_copy(
            src_ref=sends_ref.at[sides[g]], dst_ref=heard_rows.at[g],
            send_sem=row_send.at[g], recv_sem=row_recv.at[g],
            device_id=partners[g], device_id_type=MESH,
        )

    for g in range(4):
        row_copy(g).start()

    def chosen(matrix):
        return jnp.dot(pick_ref[...], matrix[...], preferred_element_type=F32).astype(BF16)

    for halo_part, far in ((halo_hi, far_hi), (halo_lo, far_lo)):
        far[...] = jnp.dot(
            halo_part[...], place_ref[...], preferred_element_type=F32
        ).astype(BF16)
    far_first_hi[...] = chosen(far_hi)
    far_first_lo[...] = chosen(far_lo)

    first, others = spans[0], pl.ds(sent, 3 * sent)
    back_hi[...] = far_first_hi[first, first]
    back_lo[...] = far_first_lo[first, first]
    echo_out[...] = back_hi[...].astype(F32) + back_lo[...].astype(F32)
    echo_copy = pltpu.make_async_remote_copy(
        src_ref=echo_out, dst_ref=echo_in, send_sem=echo_sems.at[0], recv_sem=echo_sems.at[1],
        device_id=partners[0], device_id_type=MESH,
    )
    echo_copy.start()
    own_total[...] = exact(near_hi[...], near_lo[...], counts_ref[...])
    high, low = halves(own_total[...])
    taken = jnp.dot(
        pick_ref[...], jnp.concatenate([counts_ref[...], high, low], axis=1), preferred_element_type=F32
    )
    packed_counts[...] = taken[:, :columns]
    total_ref[...] = taken[:, columns : 2 * columns] + taken[:, 2 * columns :]

    def hear_counts(g):
        row_copy(g).wait_recv()
        base = (partners[g][0] * n_sub + partners[g][1]) * rows
        heard_counts[spans[g]] = counted(base + as_column(heard_rows[g], columns)).astype(BF16)

    part = sent // 2

    def mail(slot, h, g):
        return pltpu.make_async_remote_copy(
            src_ref=outbox_ref.at[slot, h, g], dst_ref=heard_ref.at[slot, h, g],
            send_sem=send_sems.at[slot, h, g], recv_sem=recv_sems.at[slot, h, g],
            device_id=partners[g], device_id_type=MESH,
        )

    def post(slot, h, groups, fresh):
        for i, g in enumerate(groups):
            top, bottom = fresh[i * sent : i * sent + part], fresh[i * sent + part : (i + 1) * sent]
            outbox_ref[slot, h, g] = jnp.where(in_left(top), top, bottom)
        for g in groups:
            mail(slot, h, g).start()

    half = columns // 2
    sides_of = [slice(0, half), slice(half, columns)]

    def hear(slot, h, groups):
        for g in groups:
            mail(slot, h, g).wait_recv()
        for g in groups:
            for i, twice in enumerate(doubled(heard_ref[slot, h, g])):
                at = pl.ds(g * sent + i * part, part)
                if g == 0:
                    twice = twice - echo_ref[h, pl.ds(i * part, part)]
                high = twice.astype(BF16)
                rounded = high.astype(F32)
                below = twice - rounded
                heard_mixed[h, at] = jnp.where(in_left(twice), rounded, below).astype(BF16)
                low = below.astype(BF16)
                kept = sides_of[h]
                heard_pair[at, h * half : (h + 1) * half] = high[:, kept]
                heard_pair[at, columns + h * half : columns + (h + 1) * half] = low[:, kept]

    for g in (3, 2, 1, 0):
        hear_counts(g)
    keep, gain = keeps_ref[0], gains_ref[0]
    total = total_ref[...] + exact(far_first_hi[...], far_first_lo[...], heard_counts[...])
    rest = packed_counts[...] - total / centre
    residuals, directions = doubled(rest), doubled(
        keep * (packed_counts[...] / centre) + gain * rest
    )
    for h in range(2):
        packed_residual[h] = residuals[h]
        packed_direction[h] = directions[h]
        post(1, h, range(4), directions[h])

    def send_direction(direction):
        direction_ref[...] = direction
        high, low = halves(direction)
        pair_ref[:, :columns] = high
        pair_ref[:, columns:] = low

    right_side = counts_ref[...].astype(F32)
    total = own_total[...] + exact(far_hi[...], far_lo[...], heard_counts[...])
    residual = right_side - total / centre
    residual_ref[...] = residual
    before = right_side / centre
    direction = keep * before + gain * residual
    solution_ref[...] = before + direction
    send_direction(direction)

    near_first_hi[...] = chosen(near_hi)
    near_first_lo[...] = chosen(near_lo)
    far_first_hi[first, first] = jnp.zeros((sent, sent), BF16)
    far_first_lo[first, first] = jnp.zeros((sent, sent), BF16)
    echo_ref[...] = jnp.zeros((2, sent, columns), F32)
    echo_copy.wait()
    echo_hi[...], echo_lo[...] = halves(echo_in[...])

    def start_totals():
        totals = doubled(whole(near_first_hi[...], near_first_lo[...], pair_ref[...]))
        for h in range(2):
            totals_ref[h] = packed_residual[h] - totals[h]

    def far_product(at, span, h):
        return fold(product(far_first_hi[at, span], far_first_lo[at, span], heard_mixed[h, span]))

    start_totals()
    everything = pl.ds(0, packed_rows)

    def step(slot):
        keep, gain = keeps_ref[slot], gains_ref[slot]
        for h in range(2):
            hear(slot, h, (3, 2, 1))
            two = pl.ds(0, 2 * sent)
            rest = totals_ref[h, two] - far_product(two, others, h)
            packed_residual[h, two] = rest
            rest = rest[:sent]
            post(slot + 1, h, (0,), keep * packed_direction[h, first] + gain * rest)
            hear(slot, h, (0,))
            for g in (1, 2, 3):
                at = spans[g]
                if g == 1:
                    rest = packed_residual[h, at] - far_product(at, first, h)
                else:
                    rest = totals_ref[h, at] - far_product(at, everything, h)
                packed_residual[h, at] = rest
                fresh = keep * packed_direction[h, at] + gain * rest
                packed_direction[h, at] = fresh
                post(slot + 1, h, (g,), fresh)

        residual = residual_ref[...] - (
            whole(near_hi[...], near_lo[...], pair_ref[...])
            + whole(far_hi[...], far_lo[...], heard_pair[...])
        )
        residual_ref[...] = residual
        direction = keep * direction_ref[...] + gain * residual
        solution_ref[...] = solution_ref[...] + direction
        send_direction(direction)
        back = doubled(whole(back_hi[...], back_lo[...], heard_pair[first]))
        before = [packed_direction[h, first] for h in range(2)]
        high, low = halves(jnp.where(in_left(before[0]), *before))
        echo = doubled(
            gain * whole(echo_hi[...], echo_lo[...], jnp.concatenate([high, low], axis=1))
        )
        for h in range(2):
            echo_ref[h] = echo[h]
            rest = packed_residual[h, first] - back[h]
            packed_residual[h, first] = rest
            packed_direction[h, first] = keep * before[h] + gain * rest
        start_totals()

    lax.fori_loop(1, ITERS - 1, lambda slot, _: (step(slot), 0)[1], 0)

    slot = ITERS - 1
    own_total[...] = residual_ref[...] - whole(near_hi[...], near_lo[...], pair_ref[...])
    hear(slot, 0, (3, 2, 1, 0))
    for groups in ((3, 2), (1, 0)):
        hear(slot, 1, groups)
        span = pl.ds(groups[-1] * sent, len(groups) * sent)
        total = whole(far_hi[:, span], far_lo[:, span], heard_pair[span])
        if groups[-1]:
            own_total[...] = own_total[...] - total
    final = own_total[...] - total
    norms_ref[me] = jnp.sum(final * final, axis=0, keepdims=True)

    @pl.loop(1, devices)
    def _(step):
        other = lax.rem(me + step, devices)
        pltpu.make_async_remote_copy(
            src_ref=norms_ref.at[me], dst_ref=norms_ref.at[me],
            send_sem=norm_send, recv_sem=norm_recv,
            device_id=(other // n_sub, lax.rem(other, n_sub)), device_id_type=MESH,
        ).start()

    for g in range(4):
        row_copy(g).wait_send()
        for slot in range(1, ITERS):
            for h in range(2):
                mail(slot, h, g).wait_send()
    parts = norms_ref.at[pl.ds(0, devices - 1)]
    pltpu.make_async_copy(parts, parts, norm_recv).wait()
    pltpu.make_async_copy(parts, parts, norm_send).wait()
    norm_ref[...] = jnp.sqrt(jnp.sum(norms_ref[...], axis=0))


def finish(held_ref, norm_ref, result_hbm, root_hbm, sems):
    copies = [
        pltpu.make_async_copy(held_ref, result_hbm, sems.at[0]),
        pltpu.make_async_copy(norm_ref, root_hbm, sems.at[1]),
    ]
    for copy in copies:
        copy.start()
    for copy in copies:
        copy.wait()


def solution(mesh):
    n_patch, n_sub = mesh.shape["patch"], mesh.shape["sub"]

    def on_device(sources, diag_coef, tiles, tile_cols, send_rows, recv_rows, bounds):
        blk_rows, per_row, size, _ = tiles.shape
        rows = diag_coef.shape[0]
        columns = sources.shape[0]
        n_src = sources.shape[1]
        sent = send_rows.shape[2]
        halo = recv_rows.shape[1]
        packed = 4 * sent
        vmem, smem = pltpu.VMEM, pltpu.SMEM
        dma = pltpu.SemaphoreType.DMA
        anywhere = pl.BlockSpec(memory_space=pl.ANY)
        held, norm = pl.pallas_call(
            functools.partial(kernel, n_patch, n_sub),
            out_shape=(vmem((rows, columns), F32), vmem((1, columns), F32)),
            in_specs=[anywhere] * 7,
            out_specs=(pl.BlockSpec(memory_space=vmem), pl.BlockSpec(memory_space=vmem)),
            scratch_shapes=[
                vmem((n_src, columns), jnp.int32),
                vmem((blk_rows, size), F32),
                smem((blk_rows, per_row), jnp.int32),
                vmem((4, 1, sent), jnp.int32),
                vmem((1, halo), jnp.int32),
                smem((2,), F32),
                vmem(tiles.shape, F32),
                vmem((rows, rows), BF16),
                vmem((rows, rows), BF16),
                vmem((rows, packed), BF16),
                vmem((rows, packed), BF16),
                vmem((rows, halo), BF16),
                vmem((rows, halo), BF16),
                vmem((packed, rows), BF16),
                vmem((packed, rows), BF16),
                vmem((packed, packed), BF16),
                vmem((packed, packed), BF16),
                vmem((rows, columns), F32),
                vmem((rows, columns), F32),
                vmem((2, packed, columns), F32),
                vmem((2, packed, columns), F32),
                vmem((packed, columns), F32),
                vmem((2, packed, columns), F32),
                vmem((rows, columns), F32),
                vmem((rows, 2 * columns), BF16),
                vmem((packed, 2 * columns), BF16),
                vmem((2, packed, columns), BF16),
                vmem((ITERS, 2, 4, sent // 2, columns), F32),
                vmem((ITERS, 2, 4, sent // 2, columns), F32),
                vmem((4, 1, sent), jnp.int32),
                vmem((packed, columns), BF16),
                vmem((n_patch * n_sub, 1, columns), F32),
                vmem((rows, columns), BF16),
                vmem((packed, columns), F32),
                vmem((packed, rows), BF16),
                vmem((halo, packed), BF16),
                vmem((ITERS, 1, columns), F32),
                vmem((ITERS, 1, columns), F32),
                vmem((sent, sent), BF16),
                vmem((sent, sent), BF16),
                vmem((sent, sent), F32),
                vmem((sent, sent), F32),
                vmem((sent, sent), BF16),
                vmem((sent, sent), BF16),
                vmem((2, sent, columns), F32),
                dma((6,)),
                dma((blk_rows,)),
                dma((4,)),
                dma((4,)),
                dma((2,)),
                dma((ITERS, 2, 4)),
                dma((ITERS, 2, 4)),
                dma,
                dma,
            ],
            compiler_params=pltpu.CompilerParams(collective_id=0, has_side_effects=True),
            name="chebyshev",
        )(
            sources.T,
            diag_coef.reshape(blk_rows, size),
            tiles,
            tile_cols,
            send_rows.reshape(4, 1, sent),
            recv_rows,
            bounds,
        )
        result, root = pl.pallas_call(
            finish,
            out_shape=(
                jax.ShapeDtypeStruct((rows, columns), F32),
                jax.ShapeDtypeStruct((1, columns), F32),
            ),
            in_specs=[pl.BlockSpec(memory_space=vmem)] * 2,
            out_specs=(anywhere, anywhere),
            scratch_shapes=[dma((2,))],
            name="finish",
        )(pltpu.with_memory_space_constraint(held, vmem), pltpu.with_memory_space_constraint(norm, vmem))
        return result, root.reshape(columns)

    return jax.shard_map(
        on_device,
        mesh=mesh,
        in_specs=(
            P(),
            P(("patch", "sub")),
            P(("patch", "sub"), None, None, None),
            P(("patch", "sub"), None),
            P(("patch", "sub"), None, None),
            P(("patch", "sub"), None),
            P(),
        ),
        out_specs=(P(("patch", "sub"), None), P()),
        check_vma=False,
    )
```

```python
import functools

import jax
import jax.numpy as jnp
from jax import lax
from jax.experimental import pallas as pl
from jax.experimental.pallas import tpu as pltpu
from jax.sharding import PartitionSpec as P

ITERS = 8
MESH = pl.DeviceIdType.MESH
F32 = jnp.float32
BF16 = jnp.bfloat16


def halves(value):
    high = value.astype(BF16)
    return high, (value - high.astype(F32)).astype(BF16)


def product(high, low, mixed_pair):
    return jnp.dot(high, mixed_pair, preferred_element_type=F32) + jnp.dot(
        low, mixed_pair, preferred_element_type=F32
    )


def whole(high, low, pair):
    columns = pair.shape[1] // 2
    wide = jnp.dot(high, pair, preferred_element_type=F32)
    narrow = jnp.dot(low, pair[:, :columns], preferred_element_type=F32)
    return wide[:, :columns] + wide[:, columns:] + narrow


def turn(value):
    return pltpu.roll(value, value.shape[1] // 2, 1)


def in_left(value):
    lanes = lax.broadcasted_iota(jnp.int32, value.shape, 1)
    return lanes < value.shape[1] // 2


def doubled(value):
    other, left = turn(value), in_left(value)
    return jnp.where(left, value, other), jnp.where(left, other, value)


def fold(wide):
    return wide + turn(wide)


def exact(high, low, counts):
    return jnp.dot(high, counts, preferred_element_type=F32) + jnp.dot(
        low, counts, preferred_element_type=F32
    )


def kernel(
    n_patch, n_sub,
    sources_hbm, diag_hbm, tiles_hbm, cols_hbm, sends_hbm, receives_hbm, bounds_hbm,
    solution_ref, norm_ref,
    sources_ref, diag_ref, cols_ref, sends_ref, receives_ref, bounds_ref,
    tiles_ref, near_hi, near_lo, far_hi, far_lo, halo_hi, halo_lo,
    near_first_hi, near_first_lo, far_first_hi, far_first_lo,
    direction_ref, residual_ref, packed_residual, packed_direction, total_ref, totals_ref, own_total, pair_ref, heard_pair, heard_mixed,
    outbox_ref, heard_ref, heard_rows, heard_counts, norms_ref, counts_ref,
    packed_counts, pick_ref, place_ref, keeps_ref, gains_ref,
    back_hi, back_lo, echo_out, echo_in, echo_hi, echo_lo, echo_ref,
    input_sems, tile_sems, echo_sems,
    send_sems, recv_sems, norm_send, norm_recv,
):
    blk_rows, per_row, size, _ = tiles_hbm.shape
    rows = blk_rows * size
    n_src, columns = sources_ref.shape
    sent = sends_ref.shape[2]
    halo = receives_ref.shape[1]
    packed_rows = 4 * sent
    patch, sub = lax.axis_index("patch"), lax.axis_index("sub")
    devices = n_patch * n_sub
    me = patch * n_sub + sub
    patch_odd, sub_odd = lax.rem(patch, 2), lax.rem(sub, 2)

    partners = [
        (lax.rem(patch + n_patch - 1 + 2 * patch_odd, n_patch), sub),
        (lax.rem(patch + n_patch + 1 - 2 * patch_odd, n_patch), sub),
        (patch, lax.rem(sub + n_sub - 1 + 2 * sub_odd, n_sub)),
        (patch, lax.rem(sub + n_sub + 1 - 2 * sub_odd, n_sub)),
    ]
    sides = [patch_odd, 1 - patch_odd, 2 + sub_odd, 3 - sub_odd]
    spans = [pl.ds(g * sent, sent) for g in range(4)]

    barrier = pltpu.get_barrier_semaphore()
    if n_patch // 2 + n_sub // 2 <= ITERS:
        for partner in partners:
            pl.semaphore_signal(barrier, inc=1, device_id=partner, device_id_type=MESH)
        awaited = 4
    else:
        @pl.loop(1, devices)
        def _(step):
            other = lax.rem(me + step, devices)
            pl.semaphore_signal(
                barrier, inc=1, device_id=(other // n_sub, lax.rem(other, n_sub)), device_id_type=MESH
            )
        awaited = devices - 1

    inputs = [
        pltpu.make_async_copy(source, target, input_sems.at[i])
        for i, (source, target) in enumerate((
            (sends_hbm, sends_ref), (receives_hbm, receives_ref), (sources_hbm, sources_ref),
            (cols_hbm, cols_ref), (diag_hbm, diag_ref), (bounds_hbm, bounds_ref),
        ))
    ]
    for copy in inputs:
        copy.start()
    copies = [
        pltpu.make_async_copy(tiles_hbm.at[b], tiles_ref.at[b], tile_sems.at[b])
        for b in range(blk_rows)
    ]
    for copy in copies:
        copy.start()
    for copy in inputs:
        copy.wait()

    low_end = jnp.full((1, columns), bounds_ref[0], F32)
    high_end = jnp.full((1, columns), bounds_ref[1], F32)
    centre = (low_end + high_end) / 2.0
    half_width = (high_end - low_end) / 2.0
    ratio = centre / half_width
    damping = 1.0 / ratio
    for k in range(ITERS - 1):
        damping_next = 1.0 / (2.0 * ratio - damping)
        keeps_ref[k] = damping_next * damping
        gains_ref[k] = 2.0 * damping_next / half_width
        damping = damping_next

    def counted(ids):
        total = jnp.zeros(ids.shape, F32)
        for s in range(n_src):
            total = total + jnp.where(sources_ref[s : s + 1, :] == ids, 1.0, 0.0)
        return total

    counts_ref[...] = counted(
        me * rows + lax.broadcasted_iota(jnp.int32, (rows, columns), 0)
    ).astype(BF16)

    def as_column(row, width):
        return jnp.broadcast_to(row, (width, row.shape[1])).T

    for g in range(4):
        wide = as_column(sends_ref[sides[g]], rows)
        pick_ref[spans[g]] = jnp.where(
            wide == lax.broadcasted_iota(jnp.int32, (sent, rows), 1), 1.0, 0.0
        ).astype(BF16)
    for i in range(halo // size):
        wide = as_column(receives_ref[:, i * size : (i + 1) * size], sent)
        for g in range(4):
            place_ref[pl.ds(i * size, size), spans[g]] = jnp.where(
                wide == sides[g] * sent + lax.broadcasted_iota(jnp.int32, (size, sent), 1), 1.0, 0.0
            ).astype(BF16)

    eye = lax.broadcasted_iota(jnp.int32, (size, size), 0) == lax.broadcasted_iota(
        jnp.int32, (size, size), 1
    )
    for b in range(blk_rows):
        copies[b].wait()
        for c in range(blk_rows + halo // size):
            block = jnp.zeros((size, size), F32)
            for n in range(per_row):
                block = block + tiles_ref[b, n] * (cols_ref[b, n] == c).astype(F32)
            if c == b:
                block = block + jnp.where(eye, diag_ref[b : b + 1, :], 0.0)
            high, low = halves(block)
            at = pl.ds(b * size, size)
            if c < blk_rows:
                near_hi[at, pl.ds(c * size, size)] = high
                near_lo[at, pl.ds(c * size, size)] = low
            else:
                place_at = pl.ds((c - blk_rows) * size, size)
                halo_hi[at, place_at] = high
                halo_lo[at, place_at] = low

    pl.semaphore_wait(barrier, awaited)

    def arrival(slot, h, g):
        if g == 0:
            return recv_sems.at[2 * lax.rem(slot, 4) + h]
        return recv_sems.at[8 + 3 * (2 * lax.rem(slot, 2) + h) + g - 1]

    def row_copy(g):
        return pltpu.make_async_remote_copy(
            src_ref=sends_ref.at[sides[g]], dst_ref=heard_rows.at[g],
            send_sem=send_sems.at[0, g], recv_sem=arrival(0, 0, g),
            device_id=partners[g], device_id_type=MESH,
        )

    for g in range(4):
        row_copy(g).start()

    def chosen(matrix):
        return jnp.dot(pick_ref[...], matrix[...], preferred_element_type=F32).astype(BF16)

    for halo_part, far in ((halo_hi, far_hi), (halo_lo, far_lo)):
        far[...] = jnp.dot(
            halo_part[...], place_ref[...], preferred_element_type=F32
        ).astype(BF16)
    far_first_hi[...] = chosen(far_hi)
    far_first_lo[...] = chosen(far_lo)

    first, others = spans[0], pl.ds(sent, 3 * sent)
    back_hi[...] = far_first_hi[first, first]
    back_lo[...] = far_first_lo[first, first]
    echo_out[...] = back_hi[...].astype(F32) + back_lo[...].astype(F32)
    echo_copy = pltpu.make_async_remote_copy(
        src_ref=echo_out, dst_ref=echo_in, send_sem=echo_sems.at[0], recv_sem=echo_sems.at[1],
        device_id=partners[0], device_id_type=MESH,
    )
    echo_copy.start()
    own_total[...] = exact(near_hi[...], near_lo[...], counts_ref[...])
    high, low = halves(own_total[...])
    taken = jnp.dot(
        pick_ref[...], jnp.concatenate([counts_ref[...], high, low], axis=1), preferred_element_type=F32
    )
    packed_counts[...] = taken[:, :columns]
    total_ref[...] = taken[:, columns : 2 * columns] + taken[:, 2 * columns :]

    def hear_counts(g):
        row_copy(g).wait_recv()
        base = (partners[g][0] * n_sub + partners[g][1]) * rows
        heard_counts[spans[g]] = counted(base + as_column(heard_rows[g], columns)).astype(BF16)

    part = sent // 2

    def mail(slot, h, g):
        return pltpu.make_async_remote_copy(
            src_ref=outbox_ref.at[slot, h, g], dst_ref=heard_ref.at[slot, h, g],
            send_sem=send_sems.at[h, g], recv_sem=arrival(slot, h, g),
            device_id=partners[g], device_id_type=MESH,
        )

    def post(slot, h, groups, fresh, begins=False):
        for i, g in enumerate(groups):
            top, bottom = fresh[i * sent : i * sent + part], fresh[i * sent + part : (i + 1) * sent]
            outbox_ref[slot, h, g] = jnp.where(in_left(top), top, bottom)
        for g in groups:
            if not begins:
                mail(slot - 1, h, g).wait_send()
            elif h == 0:
                row_copy(g).wait_send()
            mail(slot, h, g).start()

    half = columns // 2
    sides_of = [slice(0, half), slice(half, columns)]

    def hear(slot, h, groups):
        for g in groups:
            mail(slot, h, g).wait_recv()
        for g in groups:
            for i, twice in enumerate(doubled(heard_ref[slot, h, g])):
                at = pl.ds(g * sent + i * part, part)
                if g == 0:
                    twice = twice - echo_ref[h, pl.ds(i * part, part)]
                high = twice.astype(BF16)
                rounded = high.astype(F32)
                below = twice - rounded
                heard_mixed[h, at] = jnp.where(in_left(twice), rounded, below).astype(BF16)
                low = below.astype(BF16)
                kept = sides_of[h]
                heard_pair[at, h * half : (h + 1) * half] = high[:, kept]
                heard_pair[at, columns + h * half : columns + (h + 1) * half] = low[:, kept]

    for g in (3, 2, 1, 0):
        hear_counts(g)
    keep, gain = keeps_ref[0], gains_ref[0]
    total = total_ref[...] + exact(far_first_hi[...], far_first_lo[...], heard_counts[...])
    rest = packed_counts[...] - total / centre
    residuals, directions = doubled(rest), doubled(
        keep * (packed_counts[...] / centre) + gain * rest
    )
    for h in range(2):
        packed_residual[h] = residuals[h]
        packed_direction[h] = directions[h]
        post(1, h, range(4), directions[h], True)

    def send_direction(direction):
        direction_ref[...] = direction
        high, low = halves(direction)
        pair_ref[:, :columns] = high
        pair_ref[:, columns:] = low

    right_side = counts_ref[...].astype(F32)
    total = own_total[...] + exact(far_hi[...], far_lo[...], heard_counts[...])
    residual = right_side - total / centre
    residual_ref[...] = residual
    before = right_side / centre
    direction = keep * before + gain * residual
    solution_ref[...] = before + direction
    send_direction(direction)

    near_first_hi[...] = chosen(near_hi)
    near_first_lo[...] = chosen(near_lo)
    far_first_hi[first, first] = jnp.zeros((sent, sent), BF16)
    far_first_lo[first, first] = jnp.zeros((sent, sent), BF16)
    echo_ref[...] = jnp.zeros((2, sent, columns), F32)
    echo_copy.wait()
    echo_hi[...], echo_lo[...] = halves(echo_in[...])

    def start_totals():
        totals = doubled(whole(near_first_hi[...], near_first_lo[...], pair_ref[...]))
        for h in range(2):
            totals_ref[h] = packed_residual[h] - totals[h]

    def far_product(at, span, h):
        return fold(product(far_first_hi[at, span], far_first_lo[at, span], heard_mixed[h, span]))

    start_totals()
    everything = pl.ds(0, packed_rows)

    def step(slot):
        keep, gain = keeps_ref[slot], gains_ref[slot]
        for h in range(2):
            hear(slot, h, (3, 2, 1))
            two = pl.ds(0, 2 * sent)
            rest = totals_ref[h, two] - far_product(two, others, h)
            packed_residual[h, two] = rest
            rest = rest[:sent]
            post(slot + 1, h, (0,), keep * packed_direction[h, first] + gain * rest)
            hear(slot, h, (0,))
            for g in (1, 2, 3):
                at = spans[g]
                if g == 1:
                    rest = packed_residual[h, at] - far_product(at, first, h)
                else:
                    rest = totals_ref[h, at] - far_product(at, everything, h)
                packed_residual[h, at] = rest
                fresh = keep * packed_direction[h, at] + gain * rest
                packed_direction[h, at] = fresh
                post(slot + 1, h, (g,), fresh)

        residual = residual_ref[...] - (
            whole(near_hi[...], near_lo[...], pair_ref[...])
            + whole(far_hi[...], far_lo[...], heard_pair[...])
        )
        residual_ref[...] = residual
        direction = keep * direction_ref[...] + gain * residual
        solution_ref[...] = solution_ref[...] + direction
        send_direction(direction)
        back = doubled(whole(back_hi[...], back_lo[...], heard_pair[first]))
        before = [packed_direction[h, first] for h in range(2)]
        high, low = halves(jnp.where(in_left(before[0]), *before))
        echo = doubled(
            gain * whole(echo_hi[...], echo_lo[...], jnp.concatenate([high, low], axis=1))
        )
        for h in range(2):
            echo_ref[h] = echo[h]
            rest = packed_residual[h, first] - back[h]
            packed_residual[h, first] = rest
            packed_direction[h, first] = keep * before[h] + gain * rest
        start_totals()

    lax.fori_loop(1, ITERS - 1, lambda slot, _: (step(slot), 0)[1], 0)

    slot = ITERS - 1
    own_total[...] = residual_ref[...] - whole(near_hi[...], near_lo[...], pair_ref[...])
    hear(slot, 0, (3, 2, 1, 0))
    for groups in ((3, 2), (1, 0)):
        hear(slot, 1, groups)
        span = pl.ds(groups[-1] * sent, len(groups) * sent)
        total = whole(far_hi[:, span], far_lo[:, span], heard_pair[span])
        if groups[-1]:
            own_total[...] = own_total[...] - total
    final = own_total[...] - total
    norms_ref[me] = jnp.sum(final * final, axis=0, keepdims=True)

    @pl.loop(1, devices)
    def _(step):
        other = lax.rem(me + step, devices)
        pltpu.make_async_remote_copy(
            src_ref=norms_ref.at[me], dst_ref=norms_ref.at[me],
            send_sem=norm_send, recv_sem=norm_recv,
            device_id=(other // n_sub, lax.rem(other, n_sub)), device_id_type=MESH,
        ).start()

    for g in range(4):
        for h in range(2):
            mail(ITERS - 1, h, g).wait_send()
    parts = norms_ref.at[pl.ds(0, devices - 1)]
    pltpu.make_async_copy(parts, parts, norm_recv).wait()
    pltpu.make_async_copy(parts, parts, norm_send).wait()
    norm_ref[...] = jnp.sqrt(jnp.sum(norms_ref[...], axis=0))


def finish(held_ref, norm_ref, result_hbm, root_hbm, sems):
    copies = [
        pltpu.make_async_copy(held_ref, result_hbm, sems.at[0]),
        pltpu.make_async_copy(norm_ref, root_hbm, sems.at[1]),
    ]
    for copy in copies:
        copy.start()
    for copy in copies:
        copy.wait()


def solution(mesh):
    n_patch, n_sub = mesh.shape["patch"], mesh.shape["sub"]

    def on_device(sources, diag_coef, tiles, tile_cols, send_rows, recv_rows, bounds):
        blk_rows, per_row, size, _ = tiles.shape
        rows = diag_coef.shape[0]
        columns = sources.shape[0]
        n_src = sources.shape[1]
        sent = send_rows.shape[2]
        halo = recv_rows.shape[1]
        packed = 4 * sent
        vmem, smem = pltpu.VMEM, pltpu.SMEM
        dma = pltpu.SemaphoreType.DMA
        anywhere = pl.BlockSpec(memory_space=pl.ANY)
        held, norm = pl.pallas_call(
            functools.partial(kernel, n_patch, n_sub),
            out_shape=(vmem((rows, columns), F32), vmem((1, columns), F32)),
            in_specs=[anywhere] * 7,
            out_specs=(pl.BlockSpec(memory_space=vmem), pl.BlockSpec(memory_space=vmem)),
            scratch_shapes=[
                vmem((n_src, columns), jnp.int32),
                vmem((blk_rows, size), F32),
                smem((blk_rows, per_row), jnp.int32),
                vmem((4, 1, sent), jnp.int32),
                vmem((1, halo), jnp.int32),
                smem((2,), F32),
                vmem(tiles.shape, F32),
                vmem((rows, rows), BF16),
                vmem((rows, rows), BF16),
                vmem((rows, packed), BF16),
                vmem((rows, packed), BF16),
                vmem((rows, halo), BF16),
                vmem((rows, halo), BF16),
                vmem((packed, rows), BF16),
                vmem((packed, rows), BF16),
                vmem((packed, packed), BF16),
                vmem((packed, packed), BF16),
                vmem((rows, columns), F32),
                vmem((rows, columns), F32),
                vmem((2, packed, columns), F32),
                vmem((2, packed, columns), F32),
                vmem((packed, columns), F32),
                vmem((2, packed, columns), F32),
                vmem((rows, columns), F32),
                vmem((rows, 2 * columns), BF16),
                vmem((packed, 2 * columns), BF16),
                vmem((2, packed, columns), BF16),
                vmem((ITERS, 2, 4, sent // 2, columns), F32),
                vmem((ITERS, 2, 4, sent // 2, columns), F32),
                vmem((4, 1, sent), jnp.int32),
                vmem((packed, columns), BF16),
                vmem((n_patch * n_sub, 1, columns), F32),
                vmem((rows, columns), BF16),
                vmem((packed, columns), F32),
                vmem((packed, rows), BF16),
                vmem((halo, packed), BF16),
                vmem((ITERS, 1, columns), F32),
                vmem((ITERS, 1, columns), F32),
                vmem((sent, sent), BF16),
                vmem((sent, sent), BF16),
                vmem((sent, sent), F32),
                vmem((sent, sent), F32),
                vmem((sent, sent), BF16),
                vmem((sent, sent), BF16),
                vmem((2, sent, columns), F32),
                dma((6,)),
                dma((blk_rows,)),
                dma((2,)),
                dma((2, 4)),
                dma((20,)),
                dma,
                dma,
            ],
            compiler_params=pltpu.CompilerParams(collective_id=0, has_side_effects=True),
            name="chebyshev",
        )(
            sources.T,
            diag_coef.reshape(blk_rows, size),
            tiles,
            tile_cols,
            send_rows.reshape(4, 1, sent),
            recv_rows,
            bounds,
        )
        result, root = pl.pallas_call(
            finish,
            out_shape=(
                jax.ShapeDtypeStruct((rows, columns), F32),
                jax.ShapeDtypeStruct((1, columns), F32),
            ),
            in_specs=[pl.BlockSpec(memory_space=vmem)] * 2,
            out_specs=(anywhere, anywhere),
            scratch_shapes=[dma((2,))],
            name="finish",
        )(pltpu.with_memory_space_constraint(held, vmem), pltpu.with_memory_space_constraint(norm, vmem))
        return result, root.reshape(columns)

    return jax.shard_map(
        on_device,
        mesh=mesh,
        in_specs=(
            P(),
            P(("patch", "sub")),
            P(("patch", "sub"), None, None, None),
            P(("patch", "sub"), None),
            P(("patch", "sub"), None, None),
            P(("patch", "sub"), None),
            P(),
        ),
        out_specs=(P(("patch", "sub"), None), P()),
        check_vma=False,
    )
```

```python
import functools

import jax
import jax.numpy as jnp
from jax import lax
from jax.experimental import pallas as pl
from jax.experimental.pallas import tpu as pltpu
from jax.sharding import PartitionSpec as P

ITERS = 8
MESH = pl.DeviceIdType.MESH
F32 = jnp.float32
BF16 = jnp.bfloat16


def halves(value):
    high = value.astype(BF16)
    return high, (value - high.astype(F32)).astype(BF16)


def product(high, low, mixed_pair):
    return jnp.dot(high, mixed_pair, preferred_element_type=F32) + jnp.dot(
        low, mixed_pair, preferred_element_type=F32
    )


def whole(high, low, pair):
    columns = pair.shape[1] // 2
    wide = jnp.dot(high, pair, preferred_element_type=F32)
    narrow = jnp.dot(low, pair[:, :columns], preferred_element_type=F32)
    return wide[:, :columns] + wide[:, columns:] + narrow


def turn(value):
    return pltpu.roll(value, value.shape[1] // 2, 1)


def in_left(value):
    lanes = lax.broadcasted_iota(jnp.int32, value.shape, 1)
    return lanes < value.shape[1] // 2


def doubled(value):
    other, left = turn(value), in_left(value)
    return jnp.where(left, value, other), jnp.where(left, other, value)


def fold(wide):
    return wide + turn(wide)


def exact(high, low, counts):
    return jnp.dot(high, counts, preferred_element_type=F32) + jnp.dot(
        low, counts, preferred_element_type=F32
    )


def kernel(
    n_patch, n_sub,
    sources_hbm, diag_hbm, tiles_hbm, cols_hbm, sends_hbm, receives_hbm, bounds_hbm,
    solution_ref, norm_ref,
    sources_ref, diag_ref, cols_ref, sends_ref, receives_ref, bounds_ref,
    tiles_ref, near_hi, near_lo, far_hi, far_lo, halo_hi, halo_lo,
    near_first_hi, near_first_lo, far_first_hi, far_first_lo,
    direction_ref, residual_ref, packed_residual, packed_direction, total_ref, totals_ref, own_total, pair_ref, heard_pair, heard_mixed,
    outbox_ref, heard_ref, heard_rows, heard_counts, norms_ref, counts_ref,
    packed_counts, pick_ref, place_ref, keeps_ref, gains_ref,
    back_hi, back_lo, echo_out, echo_in, echo_hi, echo_lo, echo_ref,
    input_sems, tile_sems, echo_sems,
    send_sems, recv_sems, norm_send, norm_recv,
):
    blk_rows, per_row, size, _ = tiles_hbm.shape
    rows = blk_rows * size
    n_src, columns = sources_ref.shape
    sent = sends_ref.shape[2]
    halo = receives_ref.shape[1]
    packed_rows = 4 * sent
    patch, sub = lax.axis_index("patch"), lax.axis_index("sub")
    devices = n_patch * n_sub
    me = patch * n_sub + sub
    patch_odd, sub_odd = lax.rem(patch, 2), lax.rem(sub, 2)

    partners = [
        (lax.rem(patch + n_patch - 1 + 2 * patch_odd, n_patch), sub),
        (lax.rem(patch + n_patch + 1 - 2 * patch_odd, n_patch), sub),
        (patch, lax.rem(sub + n_sub - 1 + 2 * sub_odd, n_sub)),
        (patch, lax.rem(sub + n_sub + 1 - 2 * sub_odd, n_sub)),
    ]
    sides = [patch_odd, 1 - patch_odd, 2 + sub_odd, 3 - sub_odd]
    spans = [pl.ds(g * sent, sent) for g in range(4)]

    barrier = pltpu.get_barrier_semaphore()
    if n_patch // 2 + n_sub // 2 <= ITERS:
        for partner in partners:
            pl.semaphore_signal(barrier, inc=1, device_id=partner, device_id_type=MESH)
        awaited = 4
    else:
        @pl.loop(1, devices)
        def _(step):
            other = lax.rem(me + step, devices)
            pl.semaphore_signal(
                barrier, inc=1, device_id=(other // n_sub, lax.rem(other, n_sub)), device_id_type=MESH
            )
        awaited = devices - 1

    inputs = [
        pltpu.make_async_copy(source, target, input_sems.at[i])
        for i, (source, target) in enumerate((
            (sends_hbm, sends_ref), (receives_hbm, receives_ref), (sources_hbm, sources_ref),
            (cols_hbm, cols_ref), (diag_hbm, diag_ref), (bounds_hbm, bounds_ref),
        ))
    ]
    for copy in inputs:
        copy.start()
    copies = [
        pltpu.make_async_copy(tiles_hbm.at[b], tiles_ref.at[b], tile_sems.at[b])
        for b in range(blk_rows)
    ]
    for copy in copies:
        copy.start()
    def counted(ids):
        total = jnp.zeros(ids.shape, F32)
        for s in range(n_src):
            total = total + jnp.where(sources_ref[s : s + 1, :] == ids, 1.0, 0.0)
        return total

    def as_column(row, width):
        return jnp.broadcast_to(row, (width, row.shape[1])).T

    inputs[0].wait()
    for g in range(4):
        wide = as_column(sends_ref[sides[g]], rows)
        pick_ref[spans[g]] = jnp.where(
            wide == lax.broadcasted_iota(jnp.int32, (sent, rows), 1), 1.0, 0.0
        ).astype(BF16)
    inputs[1].wait()
    for i in range(halo // size):
        wide = as_column(receives_ref[:, i * size : (i + 1) * size], sent)
        for g in range(4):
            place_ref[pl.ds(i * size, size), spans[g]] = jnp.where(
                wide == sides[g] * sent + lax.broadcasted_iota(jnp.int32, (size, sent), 1), 1.0, 0.0
            ).astype(BF16)

    inputs[2].wait()
    counts_ref[...] = counted(
        me * rows + lax.broadcasted_iota(jnp.int32, (rows, columns), 0)
    ).astype(BF16)

    for copy in inputs[3:]:
        copy.wait()
    low_end = jnp.full((1, columns), bounds_ref[0], F32)
    high_end = jnp.full((1, columns), bounds_ref[1], F32)
    centre = (low_end + high_end) / 2.0
    half_width = (high_end - low_end) / 2.0
    ratio = centre / half_width
    damping = 1.0 / ratio
    for k in range(ITERS - 1):
        damping_next = 1.0 / (2.0 * ratio - damping)
        keeps_ref[k] = damping_next * damping
        gains_ref[k] = 2.0 * damping_next / half_width
        damping = damping_next

    eye = lax.broadcasted_iota(jnp.int32, (size, size), 0) == lax.broadcasted_iota(
        jnp.int32, (size, size), 1
    )
    for b in range(blk_rows):
        copies[b].wait()
        for c in range(blk_rows + halo // size):
            block = jnp.zeros((size, size), F32)
            for n in range(per_row):
                block = block + tiles_ref[b, n] * (cols_ref[b, n] == c).astype(F32)
            if c == b:
                block = block + jnp.where(eye, diag_ref[b : b + 1, :], 0.0)
            high, low = halves(block)
            at = pl.ds(b * size, size)
            if c < blk_rows:
                near_hi[at, pl.ds(c * size, size)] = high
                near_lo[at, pl.ds(c * size, size)] = low
            else:
                place_at = pl.ds((c - blk_rows) * size, size)
                halo_hi[at, place_at] = high
                halo_lo[at, place_at] = low

    pl.semaphore_wait(barrier, awaited)

    def arrival(slot, h, g):
        if g == 0:
            return recv_sems.at[2 * lax.rem(slot, 4) + h]
        return recv_sems.at[8 + 3 * (2 * lax.rem(slot, 2) + h) + g - 1]

    def row_copy(g):
        return pltpu.make_async_remote_copy(
            src_ref=sends_ref.at[sides[g]], dst_ref=heard_rows.at[g],
            send_sem=send_sems.at[0, g], recv_sem=arrival(0, 0, g),
            device_id=partners[g], device_id_type=MESH,
        )

    for g in range(4):
        row_copy(g).start()

    def chosen(matrix):
        return jnp.dot(pick_ref[...], matrix[...], preferred_element_type=F32).astype(BF16)

    for halo_part, far in ((halo_hi, far_hi), (halo_lo, far_lo)):
        far[...] = jnp.dot(
            halo_part[...], place_ref[...], preferred_element_type=F32
        ).astype(BF16)
    far_first_hi[...] = chosen(far_hi)
    far_first_lo[...] = chosen(far_lo)

    first, others = spans[0], pl.ds(sent, 3 * sent)
    back_hi[...] = far_first_hi[first, first]
    back_lo[...] = far_first_lo[first, first]
    echo_out[...] = back_hi[...].astype(F32) + back_lo[...].astype(F32)
    echo_copy = pltpu.make_async_remote_copy(
        src_ref=echo_out, dst_ref=echo_in, send_sem=echo_sems.at[0], recv_sem=echo_sems.at[1],
        device_id=partners[0], device_id_type=MESH,
    )
    echo_copy.start()
    own_total[...] = exact(near_hi[...], near_lo[...], counts_ref[...])
    high, low = halves(own_total[...])
    taken = jnp.dot(
        pick_ref[...], jnp.concatenate([counts_ref[...], high, low], axis=1), preferred_element_type=F32
    )
    packed_counts[...] = taken[:, :columns]
    total_ref[...] = taken[:, columns : 2 * columns] + taken[:, 2 * columns :]

    def hear_counts(g):
        row_copy(g).wait_recv()
        base = (partners[g][0] * n_sub + partners[g][1]) * rows
        heard_counts[spans[g]] = counted(base + as_column(heard_rows[g], columns)).astype(BF16)

    part = sent // 2

    def mail(slot, h, g):
        return pltpu.make_async_remote_copy(
            src_ref=outbox_ref.at[slot, h, g], dst_ref=heard_ref.at[slot, h, g],
            send_sem=send_sems.at[h, g], recv_sem=arrival(slot, h, g),
            device_id=partners[g], device_id_type=MESH,
        )

    def post(slot, h, groups, fresh, begins=False):
        for i, g in enumerate(groups):
            top, bottom = fresh[i * sent : i * sent + part], fresh[i * sent + part : (i + 1) * sent]
            outbox_ref[slot, h, g] = jnp.where(in_left(top), top, bottom)
        for g in groups:
            if not begins:
                mail(slot - 1, h, g).wait_send()
            elif h == 0:
                row_copy(g).wait_send()
            mail(slot, h, g).start()

    half = columns // 2
    sides_of = [slice(0, half), slice(half, columns)]

    def hear(slot, h, groups):
        for g in groups:
            mail(slot, h, g).wait_recv()
        for g in groups:
            for i, twice in enumerate(doubled(heard_ref[slot, h, g])):
                at = pl.ds(g * sent + i * part, part)
                if g == 0:
                    twice = twice - echo_ref[h, pl.ds(i * part, part)]
                high = twice.astype(BF16)
                rounded = high.astype(F32)
                below = twice - rounded
                heard_mixed[h, at] = jnp.where(in_left(twice), rounded, below).astype(BF16)
                low = below.astype(BF16)
                kept = sides_of[h]
                heard_pair[at, h * half : (h + 1) * half] = high[:, kept]
                heard_pair[at, columns + h * half : columns + (h + 1) * half] = low[:, kept]

    for g in (3, 2, 1, 0):
        hear_counts(g)
    keep, gain = keeps_ref[0], gains_ref[0]
    total = total_ref[...] + exact(far_first_hi[...], far_first_lo[...], heard_counts[...])
    rest = packed_counts[...] - total / centre
    residuals, directions = doubled(rest), doubled(
        keep * (packed_counts[...] / centre) + gain * rest
    )
    for h in range(2):
        packed_residual[h] = residuals[h]
        packed_direction[h] = directions[h]
        post(1, h, range(4), directions[h], True)

    def send_direction(direction):
        direction_ref[...] = direction
        high, low = halves(direction)
        pair_ref[:, :columns] = high
        pair_ref[:, columns:] = low

    right_side = counts_ref[...].astype(F32)
    total = own_total[...] + exact(far_hi[...], far_lo[...], heard_counts[...])
    residual = right_side - total / centre
    residual_ref[...] = residual
    before = right_side / centre
    direction = keep * before + gain * residual
    solution_ref[...] = before + direction
    send_direction(direction)

    near_first_hi[...] = chosen(near_hi)
    near_first_lo[...] = chosen(near_lo)
    far_first_hi[first, first] = jnp.zeros((sent, sent), BF16)
    far_first_lo[first, first] = jnp.zeros((sent, sent), BF16)
    echo_ref[...] = jnp.zeros((2, sent, columns), F32)
    echo_copy.wait()
    echo_hi[...], echo_lo[...] = halves(echo_in[...])

    def start_totals():
        totals = doubled(whole(near_first_hi[...], near_first_lo[...], pair_ref[...]))
        for h in range(2):
            totals_ref[h] = packed_residual[h] - totals[h]

    def far_product(at, span, h):
        return fold(product(far_first_hi[at, span], far_first_lo[at, span], heard_mixed[h, span]))

    start_totals()
    everything = pl.ds(0, packed_rows)

    def step(slot):
        keep, gain = keeps_ref[slot], gains_ref[slot]
        for h in range(2):
            hear(slot, h, (3, 2, 1))
            two = pl.ds(0, 2 * sent)
            rest = totals_ref[h, two] - far_product(two, others, h)
            packed_residual[h, two] = rest
            rest = rest[:sent]
            post(slot + 1, h, (0,), keep * packed_direction[h, first] + gain * rest)
            hear(slot, h, (0,))
            for g in (1, 2, 3):
                at = spans[g]
                if g == 1:
                    rest = packed_residual[h, at] - far_product(at, first, h)
                else:
                    rest = totals_ref[h, at] - far_product(at, everything, h)
                packed_residual[h, at] = rest
                fresh = keep * packed_direction[h, at] + gain * rest
                packed_direction[h, at] = fresh
                post(slot + 1, h, (g,), fresh)

        residual = residual_ref[...] - (
            whole(near_hi[...], near_lo[...], pair_ref[...])
            + whole(far_hi[...], far_lo[...], heard_pair[...])
        )
        residual_ref[...] = residual
        direction = keep * direction_ref[...] + gain * residual
        solution_ref[...] = solution_ref[...] + direction
        send_direction(direction)
        back = doubled(whole(back_hi[...], back_lo[...], heard_pair[first]))
        before = [packed_direction[h, first] for h in range(2)]
        high, low = halves(jnp.where(in_left(before[0]), *before))
        echo = doubled(
            gain * whole(echo_hi[...], echo_lo[...], jnp.concatenate([high, low], axis=1))
        )
        for h in range(2):
            echo_ref[h] = echo[h]
            rest = packed_residual[h, first] - back[h]
            packed_residual[h, first] = rest
            packed_direction[h, first] = keep * before[h] + gain * rest
        start_totals()

    lax.fori_loop(1, ITERS - 1, lambda slot, _: (step(slot), 0)[1], 0)

    slot = ITERS - 1
    own_total[...] = residual_ref[...] - whole(near_hi[...], near_lo[...], pair_ref[...])
    hear(slot, 0, (3, 2, 1, 0))
    for groups in ((3, 2), (1, 0)):
        hear(slot, 1, groups)
        span = pl.ds(groups[-1] * sent, len(groups) * sent)
        total = whole(far_hi[:, span], far_lo[:, span], heard_pair[span])
        if groups[-1]:
            own_total[...] = own_total[...] - total
    final = own_total[...] - total
    norms_ref[me] = jnp.sum(final * final, axis=0, keepdims=True)

    @pl.loop(1, devices)
    def _(step):
        other = lax.rem(me + step, devices)
        pltpu.make_async_remote_copy(
            src_ref=norms_ref.at[me], dst_ref=norms_ref.at[me],
            send_sem=norm_send, recv_sem=norm_recv,
            device_id=(other // n_sub, lax.rem(other, n_sub)), device_id_type=MESH,
        ).start()

    for g in range(4):
        for h in range(2):
            mail(ITERS - 1, h, g).wait_send()
    parts = norms_ref.at[pl.ds(0, devices - 1)]
    pltpu.make_async_copy(parts, parts, norm_recv).wait()
    pltpu.make_async_copy(parts, parts, norm_send).wait()
    norm_ref[...] = jnp.sqrt(jnp.sum(norms_ref[...], axis=0))


def finish(held_ref, norm_ref, result_hbm, root_hbm, sems):
    copies = [
        pltpu.make_async_copy(held_ref, result_hbm, sems.at[0]),
        pltpu.make_async_copy(norm_ref, root_hbm, sems.at[1]),
    ]
    for copy in copies:
        copy.start()
    for copy in copies:
        copy.wait()


def solution(mesh):
    n_patch, n_sub = mesh.shape["patch"], mesh.shape["sub"]

    def on_device(sources, diag_coef, tiles, tile_cols, send_rows, recv_rows, bounds):
        blk_rows, per_row, size, _ = tiles.shape
        rows = diag_coef.shape[0]
        columns = sources.shape[0]
        n_src = sources.shape[1]
        sent = send_rows.shape[2]
        halo = recv_rows.shape[1]
        packed = 4 * sent
        vmem, smem = pltpu.VMEM, pltpu.SMEM
        dma = pltpu.SemaphoreType.DMA
        anywhere = pl.BlockSpec(memory_space=pl.ANY)
        held, norm = pl.pallas_call(
            functools.partial(kernel, n_patch, n_sub),
            out_shape=(vmem((rows, columns), F32), vmem((1, columns), F32)),
            in_specs=[anywhere] * 7,
            out_specs=(pl.BlockSpec(memory_space=vmem), pl.BlockSpec(memory_space=vmem)),
            scratch_shapes=[
                vmem((n_src, columns), jnp.int32),
                vmem((blk_rows, size), F32),
                smem((blk_rows, per_row), jnp.int32),
                vmem((4, 1, sent), jnp.int32),
                vmem((1, halo), jnp.int32),
                smem((2,), F32),
                vmem(tiles.shape, F32),
                vmem((rows, rows), BF16),
                vmem((rows, rows), BF16),
                vmem((rows, packed), BF16),
                vmem((rows, packed), BF16),
                vmem((rows, halo), BF16),
                vmem((rows, halo), BF16),
                vmem((packed, rows), BF16),
                vmem((packed, rows), BF16),
                vmem((packed, packed), BF16),
                vmem((packed, packed), BF16),
                vmem((rows, columns), F32),
                vmem((rows, columns), F32),
                vmem((2, packed, columns), F32),
                vmem((2, packed, columns), F32),
                vmem((packed, columns), F32),
                vmem((2, packed, columns), F32),
                vmem((rows, columns), F32),
                vmem((rows, 2 * columns), BF16),
                vmem((packed, 2 * columns), BF16),
                vmem((2, packed, columns), BF16),
                vmem((ITERS, 2, 4, sent // 2, columns), F32),
                vmem((ITERS, 2, 4, sent // 2, columns), F32),
                vmem((4, 1, sent), jnp.int32),
                vmem((packed, columns), BF16),
                vmem((n_patch * n_sub, 1, columns), F32),
                vmem((rows, columns), BF16),
                vmem((packed, columns), F32),
                vmem((packed, rows), BF16),
                vmem((halo, packed), BF16),
                vmem((ITERS, 1, columns), F32),
                vmem((ITERS, 1, columns), F32),
                vmem((sent, sent), BF16),
                vmem((sent, sent), BF16),
                vmem((sent, sent), F32),
                vmem((sent, sent), F32),
                vmem((sent, sent), BF16),
                vmem((sent, sent), BF16),
                vmem((2, sent, columns), F32),
                dma((6,)),
                dma((blk_rows,)),
                dma((2,)),
                dma((2, 4)),
                dma((20,)),
                dma,
                dma,
            ],
            compiler_params=pltpu.CompilerParams(collective_id=0, has_side_effects=True),
            name="chebyshev",
        )(
            sources.T,
            diag_coef.reshape(blk_rows, size),
            tiles,
            tile_cols,
            send_rows.reshape(4, 1, sent),
            recv_rows,
            bounds,
        )
        result, root = pl.pallas_call(
            finish,
            out_shape=(
                jax.ShapeDtypeStruct((rows, columns), F32),
                jax.ShapeDtypeStruct((1, columns), F32),
            ),
            in_specs=[pl.BlockSpec(memory_space=vmem)] * 2,
            out_specs=(anywhere, anywhere),
            scratch_shapes=[dma((2,))],
            name="finish",
        )(pltpu.with_memory_space_constraint(held, vmem), pltpu.with_memory_space_constraint(norm, vmem))
        return result, root.reshape(columns)

    return jax.shard_map(
        on_device,
        mesh=mesh,
        in_specs=(
            P(),
            P(("patch", "sub")),
            P(("patch", "sub"), None, None, None),
            P(("patch", "sub"), None),
            P(("patch", "sub"), None, None),
            P(("patch", "sub"), None),
            P(),
        ),
        out_specs=(P(("patch", "sub"), None), P()),
        check_vma=False,
    )
```
